32 devices in a mesh: row: 8 (over y, x, core), col: 4 (over z).
Axes of the slice: x: 2, y: 2, z: 4, core: 2. Of those that a mesh axis runs over, the one named last changes fastest.
Arguments:
- pair_state: bfloat16 [128, 128, 128], P('row', 'col'), may hold values from -6 to 6
- pair_mask: int32 [128, 128], P('row', 'col'), may hold values 0 or 1
- input_gain: float32 [2, 128], replicated, may hold values from 0.25 to 1.75
- input_bias: float32 [2, 128], replicated, may hold values from -1.5 to 1.5
- proj_weights: bfloat16 [2, 128, 512], replicated, may hold values from -0.5 to 0.5
- gate_weights: bfloat16 [2, 128, 128], replicated, may hold values from -0.5 to 0.5
- output_gain: float32 [2, 128], replicated, may hold values from 0.25 to 1.75
- output_bias: float32 [2, 128], replicated, may hold values from -1.5 to 1.5
- output_weights: bfloat16 [2, 128, 128], replicated, may hold values from -0.5 to 0.5
Outputs:
- pair_out: bfloat16 [128, 128, 128], P('row', 'col')
The draws below stay inside these ranges and needn't reach their ends.
All inputs are finite; a program needn't handle non-finite values. No bound on the sum of `pair_mask` on one device may be relied on, other than what follows from the above.
Results may differ from the reference program's by a relative error of at most 0.0058.
Values may be sent and summed in bfloat16 or wider, within the bound.
A program may use at most 64 MiB of HBM per device.

```python
import jax
import jax.numpy as jnp
from jax import lax

CZ = 128
CH = 128
NTOK = 128


def plant(result, stream_key, low, largest):
    longest = result.shape.index(max(result.shape))
    spots = []
    for shift in (0, 1):
        where = [jax.random.randint(jax.random.fold_in(stream_key, axis), (), 0, length) for axis, length in enumerate(result.shape)]
        where[longest] = (where[longest] + shift) % result.shape[longest]
        spots.append(tuple(where))
    return result.at[spots[0]].set(low).at[spots[1]].set(largest)


def shard_levels(own_key, dims, split, smallest, high):
    factor_of, own = 1.0, jax.random.fold_in(own_key, 6)
    for axis_at, parts in split:
        draws = jnp.exp(jax.random.uniform(jax.random.fold_in(own, axis_at), (parts,), jnp.float32, smallest / len(split), high / len(split)))
        factor_of = factor_of * jnp.repeat(draws, dims[axis_at] // parts).reshape([-1 if axis == axis_at else 1 for axis in range(len(dims))])
    return factor_of


def scatter_about(key, shape, scale, reach, split=(), held_as=jnp.bfloat16):
    drawn = scale * jax.random.normal(key, shape, jnp.float32)
    if split:
        drawn = drawn * shard_levels(key, shape, split, -0.22, 0.18)
    return jnp.clip(drawn, -reach, reach).astype(held_as)


def setup_inputs(seed: int = 0) -> dict:
    arg_keys = jax.random.split(jax.random.key(seed), 10)
    return {
        "pair_state": scatter_about(arg_keys[0], (NTOK, NTOK, CZ), 1.0, 6.0, ((0, 8), (1, 4))),
        "pair_mask": plant((jax.random.randint(arg_keys[1], (NTOK, NTOK), 0, 5) < 4).astype(jnp.int32), jax.random.fold_in(arg_keys[1], 1), 0, 1),
        "input_gain": jnp.clip(1.0 + 0.15 * jax.random.normal(arg_keys[2], (2, CZ), jnp.float32), 0.25, 1.75),
        "input_bias": scatter_about(arg_keys[3], (2, CZ), 0.3, 1.5, (), jnp.float32),
        "proj_weights": scatter_about(arg_keys[4], (2, CZ, 4 * CH), CZ ** -0.5, 0.5),
        "gate_weights": scatter_about(arg_keys[5], (2, CZ, CZ), CZ ** -0.5, 0.5),
        "output_gain": jnp.clip(1.0 + 0.15 * jax.random.normal(arg_keys[6], (2, CH), jnp.float32), 0.25, 1.75),
        "output_bias": scatter_about(arg_keys[7], (2, CH), 0.3, 1.5, (), jnp.float32),
        "output_weights": scatter_about(arg_keys[8], (2, CH, CZ), CH ** -0.5, 0.5),
    }


epsilon = 1e-05
group_width = 16

def normalize(values, weight_scale, weight_shift, reduce_axis):
    average = lax.optimization_barrier(jnp.mean(values, axis=reduce_axis, keepdims=True))
    centred = values - average
    spread = lax.optimization_barrier(jnp.mean(centred * centred, axis=reduce_axis, keepdims=True))
    return centred * lax.rsqrt(spread + epsilon) * weight_scale + weight_shift

def triangle(current, mask_float, layer_index, input_gain, input_bias, proj_weights, gate_weights, output_gain, output_bias, output_weights):
    pair_ln = normalize(current, input_gain[layer_index], input_bias[layer_index], -1).astype(jnp.bfloat16)
    flattened = pair_ln.reshape(NTOK * NTOK, CZ)
    gate_value = jax.nn.sigmoid(jnp.dot(flattened, gate_weights[layer_index], preferred_element_type=jnp.float32)).reshape(NTOK, NTOK, CZ)
    weights = proj_weights[layer_index]

    def channel_group(group_index):
        first_col = (group_index * group_width).astype(jnp.int32)
        pieces = []
        for offset in range(4):
            columns = lax.dynamic_slice_in_dim(weights, first_col + offset * CH, group_width, 1)
            pieces.append(jnp.dot(flattened, columns, preferred_element_type=jnp.float32).reshape(NTOK, NTOK, group_width))
        left_panel = (jax.nn.sigmoid(pieces[0]) * pieces[1] * mask_float).astype(jnp.bfloat16)
        right_panel = (jax.nn.sigmoid(pieces[2]) * pieces[3] * mask_float).astype(jnp.bfloat16)
        left_panel = lax.optimization_barrier(left_panel).astype(jnp.float32)
        right_panel = lax.optimization_barrier(right_panel).astype(jnp.float32)
        if layer_index == 0:
            product = jnp.einsum('ikc,jkc->cij', left_panel, right_panel)
        else:
            product = jnp.einsum('kic,kjc->cij', left_panel, right_panel)
        return product.astype(jnp.bfloat16)
    groups = jnp.arange(CH // group_width, dtype=jnp.int32)
    product = lax.map(channel_group, groups).reshape(CH, NTOK, NTOK)
    normed = normalize(product.astype(jnp.float32), output_gain[layer_index][:, None, None], output_bias[layer_index][:, None, None], 0)
    normed = lax.optimization_barrier(normed.astype(jnp.bfloat16)).astype(jnp.float32)
    update = jnp.einsum('cij,cd->ijd', normed, output_weights[layer_index].astype(jnp.float32))
    return current + gate_value * update

def reference(pair_state, pair_mask, input_gain, input_bias, proj_weights, gate_weights, output_gain, output_bias, output_weights):
    current = pair_state.astype(jnp.float32)
    mask_float = pair_mask.astype(jnp.float32)[:, :, None]
    for layer_index in range(2):
        current = triangle(current, mask_float, layer_index, input_gain, input_bias, proj_weights, gate_weights, output_gain, output_bias, output_weights)
    return current.astype(jnp.bfloat16)
```

```python
import functools

import jax
import jax.numpy as jnp
from jax import lax
from jax.experimental import pallas as pl
from jax.experimental.pallas import tpu as pltpu
from jax.sharding import PartitionSpec as P

epsilon = 1e-05


def normalize(values, weight_scale, weight_shift, reduce_axis):
    average = jnp.mean(values, axis=reduce_axis, keepdims=True)
    centred = values - average
    spread = jnp.mean(centred * centred, axis=reduce_axis, keepdims=True)
    return centred * lax.rsqrt(spread + epsilon) * weight_scale + weight_shift


def contract(left_panel, right_panel, layer_index):
    if layer_index == 0:
        product = jnp.einsum(
            "cik,cjk->cij", left_panel, right_panel, preferred_element_type=jnp.float32
        )
    else:
        product = jnp.einsum(
            "cki,ckj->cij", left_panel, right_panel, preferred_element_type=jnp.float32
        )
    return product.astype(jnp.bfloat16)


def gated_panel(pair_ln, weights, first, hidden, mask_float):
    projected = jnp.einsum(
        "ijd,de->eij",
        pair_ln,
        weights[:, first : first + 2 * hidden],
        preferred_element_type=jnp.float32,
    )
    return (jax.nn.sigmoid(projected[:hidden]) * projected[hidden:] * mask_float).astype(
        jnp.bfloat16
    )


def on_device(
    pair_state,
    pair_mask,
    input_gain,
    input_bias,
    proj_weights,
    gate_weights,
    output_gain,
    output_bias,
    output_weights,
):
    tile_rows, tile_cols, channels = pair_state.shape
    hidden = output_weights.shape[1]
    row_count = lax.axis_size("row")
    col_count = lax.axis_size("col")
    per_device = hidden // (row_count * col_count)
    current = pair_state.astype(jnp.float32)
    mask_float = pair_mask.astype(jnp.float32)[None]
    for layer_index in range(2):
        pair_ln = normalize(current, input_gain[layer_index], input_bias[layer_index], -1).astype(
            jnp.bfloat16
        )
        left_panel = gated_panel(pair_ln, proj_weights[layer_index], 0, hidden, mask_float)
        right_panel = gated_panel(
            pair_ln, proj_weights[layer_index], 2 * hidden, hidden, mask_float
        )
        gate_value = jax.nn.sigmoid(
            jnp.einsum(
                "ijd,de->ije",
                pair_ln,
                gate_weights[layer_index],
                preferred_element_type=jnp.float32,
            )
        )
        scale_out = output_gain[layer_index]
        shift_out = output_bias[layer_index]
        weight_out = output_weights[layer_index]
        left_recv, right_recv = (
            lax.all_to_all(left_panel, ("row", "col"), split_axis=0, concat_axis=1, tiled=True),
            lax.all_to_all(right_panel, ("row", "col"), split_axis=0, concat_axis=1, tiled=True),
        )
        left_chan = (
            left_recv.reshape(per_device, row_count, col_count, tile_rows, tile_cols)
            .transpose(0, 1, 3, 2, 4)
            .reshape(per_device, row_count * tile_rows, col_count * tile_cols)
        )
        right_chan = (
            right_recv.reshape(per_device, row_count, col_count, tile_rows, tile_cols)
            .transpose(0, 1, 3, 2, 4)
            .reshape(per_device, row_count * tile_rows, col_count * tile_cols)
        )
        product = contract(left_chan, right_chan, layer_index)
        arranged = (
            product.reshape(per_device, row_count, tile_rows, col_count, tile_cols)
            .transpose(0, 1, 3, 2, 4)
            .reshape(per_device, row_count * col_count * tile_rows, tile_cols)
        )
        returned = lax.all_to_all(arranged, ("row", "col"), split_axis=1, concat_axis=0, tiled=True)
        normed = normalize(
            returned.astype(jnp.float32), scale_out[:, None, None], shift_out[:, None, None], 0
        ).astype(jnp.bfloat16)
        update = jnp.einsum("cij,cd->ijd", normed, weight_out, preferred_element_type=jnp.float32)
        current = current + gate_value * update
    return current.astype(jnp.bfloat16)


MESH = pl.DeviceIdType.MESH
F32 = jnp.float32
BF16 = jnp.bfloat16


def sigmoid(values):
    return 0.5 * jnp.tanh(0.5 * values) + 0.5


def lane_groups(shape, width):
    return lax.broadcasted_iota(jnp.int32, shape, len(shape) - 1) // width


def swap_groups(blocks, width):
    count = len(blocks)
    blocks = list(blocks)
    lanes = count * width
    group = lane_groups(blocks[0].shape, width)
    step = count // 2
    while step:
        low = (group // step) % 2 == 0
        for p in range(count):
            if p & step:
                continue
            first, second = blocks[p], blocks[p + step]
            shift = step * width
            blocks[p] = jnp.where(low, first, pltpu.roll(second, shift, 1))
            blocks[p + step] = jnp.where(low, pltpu.roll(first, lanes - shift, 1), second)
        step //= 2
    return blocks


def columns_of(row_vector, lanes):
    return jnp.transpose(jnp.broadcast_to(row_vector, (lanes, row_vector.shape[1])))


def contract_first(left, right):
    return lax.dot_general(left, right, (((0,), (0,)), ((), ())), preferred_element_type=F32)


def fused_kernel(
    row_count,
    col_count,
    z_ref,
    mask_ref,
    in_gain,
    in_bias,
    proj_ref,
    gate_ref,
    out_gain,
    out_bias,
    outw_ref,
    out_ref,
    zt_ref,
    tmp_ref,
    gain_ref,
    bias_ref,
    send1,
    recv1,
    send2,
    recv2,
    send_sem,
    recv_sem,
):
    tile_rows, tile_cols, channels = z_ref.shape
    pairs = tile_rows * tile_cols
    devices = row_count * col_count
    hidden = outw_ref.shape[1]
    own = hidden // devices
    lanes = own * tile_cols
    blocks = pairs // lanes
    tokens = row_count * tile_rows
    row, col = lax.axis_index("row"), lax.axis_index("col")
    me = row * col_count + col

    def place(step):
        target = lax.rem(me + step, devices)
        return target, target // col_count, lax.rem(target, col_count)

    barrier = pltpu.get_barrier_semaphore()

    def greet(step, carry):
        _, trow, tcol = place(step)
        pl.semaphore_signal(barrier, inc=1, device_id=(trow, tcol), device_id_type=MESH)
        return carry

    lax.fori_loop(1, devices, greet, 0)

    def copy_panels(layer, step):
        target, trow, tcol = place(step)
        return pltpu.make_async_remote_copy(
            src_ref=send1.at[layer, target],
            dst_ref=recv1.at[layer, col, row],
            send_sem=send_sem.at[2 * layer, step],
            recv_sem=recv_sem.at[2 * layer, step],
            device_id=(trow, tcol),
            device_id_type=MESH,
        )

    def copy_product(layer, step):
        target, trow, tcol = place(step)
        return pltpu.make_async_remote_copy(
            src_ref=send2.at[layer, tcol, trow],
            dst_ref=recv2.at[layer, me],
            send_sem=send_sem.at[2 * layer + 1, step],
            recv_sem=recv_sem.at[2 * layer + 1, step],
            device_id=(trow, tcol),
            device_id_type=MESH,
        )

    def start_all(make, layer):
        def body(step, carry):
            make(layer, step).start()
            return carry

        lax.fori_loop(1, devices, body, 0)

    def arrive_all(make, layer):
        def body(step, carry):
            make(layer, step).wait_recv()
            return carry

        lax.fori_loop(1, devices, body, 0)

    zt_ref[...] = jnp.transpose(z_ref[...].astype(F32).reshape(pairs, channels))
    spread = (
        lax.broadcasted_iota(jnp.int32, (tile_cols, pairs), 1) % tile_cols
        == lax.broadcasted_iota(jnp.int32, (tile_cols, pairs), 0)
    ).astype(F32)
    mine = (
        lax.broadcasted_iota(jnp.int32, (tile_rows, pairs), 1) // tile_cols
        == lax.broadcasted_iota(jnp.int32, (tile_rows, pairs), 0)
    ).astype(F32)
    mask_flat = jnp.sum(
        jnp.dot(mask_ref[...].astype(F32), spread, preferred_element_type=F32) * mine,
        axis=0,
        keepdims=True,
    )

    for layer in range(2):
        current = zt_ref[...]
        centred = current - jnp.mean(current, axis=0, keepdims=True)
        scale = lax.rsqrt(jnp.mean(centred * centred, axis=0, keepdims=True) + epsilon)
        gain = columns_of(in_gain[layer : layer + 1, :], lanes)
        bias = columns_of(in_bias[layer : layer + 1, :], lanes)
        gain = jnp.concatenate([gain] * blocks, axis=1)
        bias = jnp.concatenate([bias] * blocks, axis=1)
        normed = (centred * scale * gain + bias).astype(BF16)
        projected = contract_first(proj_ref[layer], normed)
        for side in range(2):
            first = 2 * side * hidden
            panel = (
                sigmoid(projected[first : first + hidden])
                * projected[first + hidden : first + 2 * hidden]
                * mask_flat
            )
            for block in range(blocks):
                parts = [
                    panel[k * devices : (k + 1) * devices, block * lanes : (block + 1) * lanes]
                    for k in range(own)
                ]
                for q, part in enumerate(swap_groups(parts, tile_cols)):
                    line = block * own + q
                    tmp_ref[side, line * devices : (line + 1) * devices, :] = part
            for target in range(devices):
                send1[layer, target, side] = tmp_ref[
                    side, pl.ds(target, tile_rows, stride=devices), :
                ].astype(BF16)
        if layer == 0:
            pl.semaphore_wait(barrier, devices - 1)
        start_all(copy_panels, layer)
        recv1[layer, col, row] = send1[layer, me]
        gate_value = sigmoid(contract_first(gate_ref[layer], normed))
        group = lane_groups((devices, lanes), tile_cols)
        for source, kept in ((out_gain, gain_ref), (out_bias, bias_ref)):
            wide = columns_of(source[layer : layer + 1, :], lanes)
            packed = wide[0:devices]
            for k in range(1, own):
                packed = jnp.where(group == k, wide[k * devices : (k + 1) * devices], packed)
            kept[...] = packed
        arrive_all(copy_panels, layer)

        left = jnp.concatenate(
            [recv1[layer, c, :, 0].reshape(tokens, lanes) for c in range(col_count)], axis=1
        )
        right = jnp.concatenate(
            [recv1[layer, c, :, 1].reshape(tokens, lanes) for c in range(col_count)], axis=1
        )
        if layer == 0:
            wide_group = lane_groups((1, col_count * lanes), tile_cols) % own
            masks = [(wide_group == k).astype(F32).astype(BF16) for k in range(own)]
            for c in range(col_count):
                rows = right[c * tile_cols : (c + 1) * tile_cols]
                stacked = jnp.concatenate([rows * masks[k] for k in range(own)], axis=0)
                product = lax.dot_general(
                    left, stacked, (((1,), (1,)), ((), ())), preferred_element_type=F32
                )
                send2[layer, c] = product.astype(BF16).reshape(row_count, tile_rows, lanes)
        else:
            product = contract_first(left, right)
            group = lane_groups((tile_cols, lanes), tile_cols)
            for c in range(col_count):
                pieces = []
                for d in range(col_count):
                    at = d * lanes
                    piece = product[at : at + tile_cols, c * lanes : (c + 1) * lanes]
                    for k in range(1, own):
                        low = at + k * tile_cols
                        piece = jnp.where(
                            group == k,
                            product[low : low + tile_cols, c * lanes : (c + 1) * lanes],
                            piece,
                        )
                    pieces.append(piece.astype(BF16))
                send2[layer, c] = jnp.concatenate(pieces, axis=0).reshape(
                    row_count, tile_rows, lanes
                )
        start_all(copy_product, layer)
        recv2[layer, me] = send2[layer, col, row]
        arrive_all(copy_product, layer)

        returned = recv2[layer].astype(F32)

        def over_channels(values):
            total = jnp.sum(values, axis=0)
            shift = lanes // 2
            while shift >= tile_cols:
                total = total + pltpu.roll(total, shift, 1)
                shift //= 2
            return total * (1.0 / hidden)

        centred = returned - over_channels(returned)[None]
        scale = lax.rsqrt(over_channels(centred * centred) + epsilon)
        for d in range(devices):
            tmp_ref[0, d * tile_rows : (d + 1) * tile_rows, :] = (
                centred[d] * scale * gain_ref[d : d + 1, :] + bias_ref[d : d + 1, :]
            )
        wide_blocks = []
        for block in range(blocks):
            parts = [
                tmp_ref[0, pl.ds(block * own + q, devices, stride=tile_rows), :] for q in range(own)
            ]
            wide_blocks.append(
                jnp.concatenate(swap_groups(parts, tile_cols), axis=0).astype(BF16)
            )
        update = contract_first(outw_ref[layer], jnp.concatenate(wide_blocks, axis=1))
        zt_ref[...] = zt_ref[...] + gate_value * update

    out_ref[...] = (
        jnp.transpose(zt_ref[...]).reshape(tile_rows, tile_cols, channels).astype(BF16)
    )
    for layer in range(2):
        for make in (copy_panels, copy_product):

            def body(step, carry):
                make(layer, step).wait_send()
                return carry

            lax.fori_loop(1, devices, body, 0)


def fused(row_count, col_count, *args):
    tile_rows, tile_cols, channels = args[0].shape
    devices = row_count * col_count
    hidden = args[-1].shape[1]
    lanes = hidden // devices * tile_cols
    pairs = tile_rows * tile_cols
    vmem = pl.BlockSpec(memory_space=pltpu.VMEM)
    return pl.pallas_call(
        functools.partial(fused_kernel, row_count, col_count),
        out_shape=jax.ShapeDtypeStruct(args[0].shape, BF16),
        in_specs=[vmem] * len(args),
        out_specs=vmem,
        scratch_shapes=[
            pltpu.VMEM((channels, pairs), F32),
            pltpu.VMEM((2, tile_rows * devices, lanes), F32),
            pltpu.VMEM((devices, lanes), F32),
            pltpu.VMEM((devices, lanes), F32),
            pltpu.VMEM((2, devices, 2, tile_rows, lanes), BF16),
            pltpu.VMEM((2, col_count, row_count, 2, tile_rows, lanes), BF16),
            pltpu.VMEM((2, col_count, row_count, tile_rows, lanes), BF16),
            pltpu.VMEM((2, devices, tile_rows, lanes), BF16),
            pltpu.SemaphoreType.DMA((4, devices)),
            pltpu.SemaphoreType.DMA((4, devices)),
        ],
        compiler_params=pltpu.CompilerParams(collective_id=0, has_side_effects=True),
    )(*args)


def solution(mesh):
    row_count, col_count = mesh.shape["row"], mesh.shape["col"]
    devices = row_count * col_count

    def step(*args):
        tile_rows, tile_cols, channels = args[0].shape
        hidden = args[-1].shape[1]
        own = hidden // devices
        fits = (
            hidden % devices == 0
            and own * tile_cols == 128
            and tile_rows % 16 == 0
            and tile_rows % own == 0
            and own & (own - 1) == 0
            and row_count * tile_rows == col_count * tile_cols
        )
        return fused(row_count, col_count, *args) if fits else on_device(*args)

    return jax.shard_map(
        step,
        mesh=mesh,
        in_specs=(P("row", "col", None), P("row", "col"), P(), P(), P(), P(), P(), P(), P()),
        out_specs=P("row", "col", None),
        check_vma=False,
    )
```

```python
import functools

import jax
import jax.numpy as jnp
from jax import lax
from jax.experimental import pallas as pl
from jax.experimental.pallas import tpu as pltpu
from jax.sharding import PartitionSpec as P

epsilon = 1e-05


def normalize(values, weight_scale, weight_shift, reduce_axis):
    average = jnp.mean(values, axis=reduce_axis, keepdims=True)
    centred = values - average
    spread = jnp.mean(centred * centred, axis=reduce_axis, keepdims=True)
    return centred * lax.rsqrt(spread + epsilon) * weight_scale + weight_shift


def contract(left_panel, right_panel, layer_index):
    if layer_index == 0:
        product = jnp.einsum(
            "cik,cjk->cij", left_panel, right_panel, preferred_element_type=jnp.float32
        )
    else:
        product = jnp.einsum(
            "cki,ckj->cij", left_panel, right_panel, preferred_element_type=jnp.float32
        )
    return product.astype(jnp.bfloat16)


def gated_panel(pair_ln, weights, first, hidden, mask_float):
    projected = jnp.einsum(
        "ijd,de->eij",
        pair_ln,
        weights[:, first : first + 2 * hidden],
        preferred_element_type=jnp.float32,
    )
    return (jax.nn.sigmoid(projected[:hidden]) * projected[hidden:] * mask_float).astype(
        jnp.bfloat16
    )


def on_device(
    pair_state,
    pair_mask,
    input_gain,
    input_bias,
    proj_weights,
    gate_weights,
    output_gain,
    output_bias,
    output_weights,
):
    tile_rows, tile_cols, channels = pair_state.shape
    hidden = output_weights.shape[1]
    row_count = lax.axis_size("row")
    col_count = lax.axis_size("col")
    per_device = hidden // (row_count * col_count)
    current = pair_state.astype(jnp.float32)
    mask_float = pair_mask.astype(jnp.float32)[None]
    for layer_index in range(2):
        pair_ln = normalize(current, input_gain[layer_index], input_bias[layer_index], -1).astype(
            jnp.bfloat16
        )
        left_panel = gated_panel(pair_ln, proj_weights[layer_index], 0, hidden, mask_float)
        right_panel = gated_panel(
            pair_ln, proj_weights[layer_index], 2 * hidden, hidden, mask_float
        )
        gate_value = jax.nn.sigmoid(
            jnp.einsum(
                "ijd,de->ije",
                pair_ln,
                gate_weights[layer_index],
                preferred_element_type=jnp.float32,
            )
        )
        scale_out = output_gain[layer_index]
        shift_out = output_bias[layer_index]
        weight_out = output_weights[layer_index]
        left_recv, right_recv = (
            lax.all_to_all(left_panel, ("row", "col"), split_axis=0, concat_axis=1, tiled=True),
            lax.all_to_all(right_panel, ("row", "col"), split_axis=0, concat_axis=1, tiled=True),
        )
        left_chan = (
            left_recv.reshape(per_device, row_count, col_count, tile_rows, tile_cols)
            .transpose(0, 1, 3, 2, 4)
            .reshape(per_device, row_count * tile_rows, col_count * tile_cols)
        )
        right_chan = (
            right_recv.reshape(per_device, row_count, col_count, tile_rows, tile_cols)
            .transpose(0, 1, 3, 2, 4)
            .reshape(per_device, row_count * tile_rows, col_count * tile_cols)
        )
        product = contract(left_chan, right_chan, layer_index)
        arranged = (
            product.reshape(per_device, row_count, tile_rows, col_count, tile_cols)
            .transpose(0, 1, 3, 2, 4)
            .reshape(per_device, row_count * col_count * tile_rows, tile_cols)
        )
        returned = lax.all_to_all(arranged, ("row", "col"), split_axis=1, concat_axis=0, tiled=True)
        normed = normalize(
            returned.astype(jnp.float32), scale_out[:, None, None], shift_out[:, None, None], 0
        ).astype(jnp.bfloat16)
        update = jnp.einsum("cij,cd->ijd", normed, weight_out, preferred_element_type=jnp.float32)
        current = current + gate_value * update
    return current.astype(jnp.bfloat16)


MESH = pl.DeviceIdType.MESH
F32 = jnp.float32
BF16 = jnp.bfloat16


def sigmoid(values):
    return 0.5 * jnp.tanh(0.5 * values) + 0.5


def lane_groups(shape, width):
    return lax.broadcasted_iota(jnp.int32, shape, len(shape) - 1) // width


def swap_groups(blocks, width):
    count = len(blocks)
    blocks = list(blocks)
    lanes = count * width
    group = lane_groups(blocks[0].shape, width)
    step = count // 2
    while step:
        low = (group // step) % 2 == 0
        for p in range(count):
            if p & step:
                continue
            first, second = blocks[p], blocks[p + step]
            shift = step * width
            blocks[p] = jnp.where(low, first, pltpu.roll(second, shift, 1))
            blocks[p + step] = jnp.where(low, pltpu.roll(first, lanes - shift, 1), second)
        step //= 2
    return blocks


def columns_of(row_vector, lanes):
    return jnp.transpose(jnp.broadcast_to(row_vector, (lanes, row_vector.shape[1])))


def contract_first(left, right):
    return lax.dot_general(left, right, (((0,), (0,)), ((), ())), preferred_element_type=F32)


def fused_kernel(
    row_count,
    col_count,
    *refs,
):
    operands, out_ref, held = refs[:9], refs[9], refs[10:19]
    load_sem = refs[19]
    loads = [
        pltpu.make_async_copy(source, target, load_sem.at[at])
        for at, (source, target) in enumerate(zip(operands, held))
    ]
    for at in (0, 1, 2, 3, 4, 5, 6, 7, 8):
        loads[at].start()
    fused_body(row_count, col_count, loads, *held, out_ref, *refs[20:])


def fused_body(
    row_count,
    col_count,
    loads,
    z_ref,
    mask_ref,
    in_gain,
    in_bias,
    proj_ref,
    gate_ref,
    out_gain,
    out_bias,
    outw_ref,
    out_ref,
    zt_ref,
    tmp_ref,
    gain_ref,
    bias_ref,
    send1,
    recv1,
    send2,
    recv2,
    send_sem,
    recv_sem,
):
    tile_rows, tile_cols, channels = z_ref.shape
    pairs = tile_rows * tile_cols
    devices = row_count * col_count
    hidden = outw_ref.shape[1]
    own = hidden // devices
    lanes = own * tile_cols
    blocks = pairs // lanes
    tokens = row_count * tile_rows
    row, col = lax.axis_index("row"), lax.axis_index("col")
    me = row * col_count + col

    half = col_count // 2
    near, inner = col // half, lax.rem(col, half)

    def place(turn, step):
        if turn < half:
            tcol = (1 - near) * half + lax.rem(2 * half - 1 - inner + turn, half)
            trow = lax.rem(2 * row_count - 1 - row + step, row_count)
        else:
            tcol = near * half + lax.rem(inner + 1 + turn - half, half)
            trow = lax.rem(row + 1 + step, row_count)
        return trow * col_count + tcol, trow, tcol

    def each(action):
        for turn in range(col_count):

            def body(step, carry, turn=turn):
                action(turn, step)
                return carry

            lax.fori_loop(0, row_count - (turn == col_count - 1), body, 0, unroll=True)

    barrier = pltpu.get_barrier_semaphore()

    def greet(turn, step):
        _, trow, tcol = place(turn, step)
        pl.semaphore_signal(barrier, inc=1, device_id=(trow, tcol), device_id_type=MESH)

    each(greet)

    def copy_panels(layer, turn, step):
        target, trow, tcol = place(turn, step)
        return pltpu.make_async_remote_copy(
            src_ref=send1.at[layer, target],
            dst_ref=recv1.at[layer, col, row],
            send_sem=send_sem.at[2 * layer],
            recv_sem=recv_sem.at[2 * layer],
            device_id=(trow, tcol),
            device_id_type=MESH,
        )

    def copy_product(layer, turn, step):
        target, trow, tcol = place(turn, step)
        return pltpu.make_async_remote_copy(
            src_ref=send2.at[layer, tcol, trow],
            dst_ref=recv2.at[layer, me],
            send_sem=send_sem.at[2 * layer + 1],
            recv_sem=recv_sem.at[2 * layer + 1],
            device_id=(trow, tcol),
            device_id_type=MESH,
        )

    def start_all(make, layer):
        each(lambda turn, step: make(layer, turn, step).start())

    def wait_panels(sem, layer):
        slots = send1.at[layer, pl.ds(0, devices - 1)]
        pltpu.make_async_copy(slots, slots, sem.at[2 * layer]).wait()

    def wait_products(sem, layer):
        slots = recv2.at[layer, pl.ds(0, devices - 1)]
        pltpu.make_async_copy(slots, slots, sem.at[2 * layer + 1]).wait()

    loads[0].wait()
    zt_ref[...] = jnp.transpose(z_ref[...].astype(F32).reshape(pairs, channels))
    for at in range(1, len(loads)):
        loads[at].wait()
    spread = (
        lax.broadcasted_iota(jnp.int32, (tile_cols, pairs), 1) % tile_cols
        == lax.broadcasted_iota(jnp.int32, (tile_cols, pairs), 0)
    ).astype(F32)
    mine = (
        lax.broadcasted_iota(jnp.int32, (tile_rows, pairs), 1) // tile_cols
        == lax.broadcasted_iota(jnp.int32, (tile_rows, pairs), 0)
    ).astype(F32)
    mask_flat = jnp.sum(
        jnp.dot(mask_ref[...].astype(F32), spread, preferred_element_type=F32) * mine,
        axis=0,
        keepdims=True,
    )

    for layer in range(2):
        current = zt_ref[...]
        centred = current - jnp.mean(current, axis=0, keepdims=True)
        scale = lax.rsqrt(jnp.mean(centred * centred, axis=0, keepdims=True) + epsilon)
        gain = columns_of(in_gain[layer : layer + 1, :], lanes)
        bias = columns_of(in_bias[layer : layer + 1, :], lanes)
        gain = jnp.concatenate([gain] * blocks, axis=1)
        bias = jnp.concatenate([bias] * blocks, axis=1)
        normed = (centred * scale * gain + bias).astype(BF16)
        projected = contract_first(proj_ref[layer], normed)
        for side in range(2):
            first = 2 * side * hidden
            panel = (
                sigmoid(projected[first : first + hidden])
                * projected[first + hidden : first + 2 * hidden]
                * mask_flat
            )
            for block in range(blocks):
                parts = [
                    panel[k * devices : (k + 1) * devices, block * lanes : (block + 1) * lanes]
                    for k in range(own)
                ]
                for q, part in enumerate(swap_groups(parts, tile_cols)):
                    line = block * own + q
                    tmp_ref[side, line * devices : (line + 1) * devices, :] = part
            for target in range(devices):
                send1[layer, target, side] = tmp_ref[
                    side, pl.ds(target, tile_rows, stride=devices), :
                ].astype(BF16)
        if layer == 0:
            pl.semaphore_wait(barrier, devices - 1)
        start_all(copy_panels, layer)
        recv1[layer, col, row] = send1[layer, me]
        gate_value = sigmoid(contract_first(gate_ref[layer], normed))
        group = lane_groups((devices, lanes), tile_cols)
        for source, kept in ((out_gain, gain_ref), (out_bias, bias_ref)):
            wide = columns_of(source[layer : layer + 1, :], lanes)
            packed = wide[0:devices]
            for k in range(1, own):
                packed = jnp.where(group == k, wide[k * devices : (k + 1) * devices], packed)
            kept[...] = packed
        wait_panels(recv_sem, layer)

        left = jnp.concatenate(
            [recv1[layer, c, :, 0].reshape(tokens, lanes) for c in range(col_count)], axis=1
        )
        right = jnp.concatenate(
            [recv1[layer, c, :, 1].reshape(tokens, lanes) for c in range(col_count)], axis=1
        )
        if layer == 0:
            wide_group = lane_groups((1, col_count * lanes), tile_cols) % own
            masks = [(wide_group == k).astype(F32).astype(BF16) for k in range(own)]
            for c in range(col_count):
                rows = right[c * tile_cols : (c + 1) * tile_cols]
                stacked = jnp.concatenate([rows * masks[k] for k in range(own)], axis=0)
                product = lax.dot_general(
                    left, stacked, (((1,), (1,)), ((), ())), preferred_element_type=F32
                )
                send2[layer, c] = product.astype(BF16).reshape(row_count, tile_rows, lanes)
        else:
            product = contract_first(left, right)
            group = lane_groups((tile_cols, lanes), tile_cols)
            for c in range(col_count):
                pieces = []
                for d in range(col_count):
                    at = d * lanes
                    piece = product[at : at + tile_cols, c * lanes : (c + 1) * lanes]
                    for k in range(1, own):
                        low = at + k * tile_cols
                        piece = jnp.where(
                            group == k,
                            product[low : low + tile_cols, c * lanes : (c + 1) * lanes],
                            piece,
                        )
                    pieces.append(piece.astype(BF16))
                send2[layer, c] = jnp.concatenate(pieces, axis=0).reshape(
                    row_count, tile_rows, lanes
                )
        start_all(copy_product, layer)
        recv2[layer, me] = send2[layer, col, row]
        wait_products(recv_sem, layer)

        returned = recv2[layer].astype(F32)

        def over_channels(values):
            total = jnp.sum(values, axis=0)
            shift = lanes // 2
            while shift >= tile_cols:
                total = total + pltpu.roll(total, shift, 1)
                shift //= 2
            return total * (1.0 / hidden)

        centred = returned - over_channels(returned)[None]
        scale = lax.rsqrt(over_channels(centred * centred) + epsilon)
        for d in range(devices):
            tmp_ref[0, d * tile_rows : (d + 1) * tile_rows, :] = (
                centred[d] * scale * gain_ref[d : d + 1, :] + bias_ref[d : d + 1, :]
            )
        wide_blocks = []
        for block in range(blocks):
            parts = [
                tmp_ref[0, pl.ds(block * own + q, devices, stride=tile_rows), :] for q in range(own)
            ]
            wide_blocks.append(
                jnp.concatenate(swap_groups(parts, tile_cols), axis=0).astype(BF16)
            )
        update = contract_first(outw_ref[layer], jnp.concatenate(wide_blocks, axis=1))
        zt_ref[...] = zt_ref[...] + gate_value * update

    out_ref[...] = (
        jnp.transpose(zt_ref[...]).reshape(tile_rows, tile_cols, channels).astype(BF16)
    )
    for layer in range(2):
        wait_panels(send_sem, layer)
        wait_products(send_sem, layer)


def fused(row_count, col_count, *args):
    tile_rows, tile_cols, channels = args[0].shape
    devices = row_count * col_count
    hidden = args[-1].shape[1]
    lanes = hidden // devices * tile_cols
    pairs = tile_rows * tile_cols
    vmem = pl.BlockSpec(memory_space=pltpu.VMEM)
    return pl.pallas_call(
        functools.partial(fused_kernel, row_count, col_count),
        out_shape=jax.ShapeDtypeStruct(args[0].shape, BF16),
        in_specs=[pl.BlockSpec(memory_space=pl.ANY)] * len(args),
        out_specs=vmem,
        scratch_shapes=[pltpu.VMEM(arg.shape, arg.dtype) for arg in args]
        + [
            pltpu.SemaphoreType.DMA((len(args),)),
            pltpu.VMEM((channels, pairs), F32),
            pltpu.VMEM((2, tile_rows * devices, lanes), F32),
            pltpu.VMEM((devices, lanes), F32),
            pltpu.VMEM((devices, lanes), F32),
            pltpu.VMEM((2, devices, 2, tile_rows, lanes), BF16),
            pltpu.VMEM((2, col_count, row_count, 2, tile_rows, lanes), BF16),
            pltpu.VMEM((2, col_count, row_count, tile_rows, lanes), BF16),
            pltpu.VMEM((2, devices, tile_rows, lanes), BF16),
            pltpu.SemaphoreType.DMA((4,)),
            pltpu.SemaphoreType.DMA((4,)),
        ],
        compiler_params=pltpu.CompilerParams(collective_id=0, has_side_effects=True),
    )(*args)


def solution(mesh):
    row_count, col_count = mesh.shape["row"], mesh.shape["col"]
    devices = row_count * col_count

    def step(*args):
        tile_rows, tile_cols, channels = args[0].shape
        hidden = args[-1].shape[1]
        own = hidden // devices
        fits = (
            hidden % devices == 0
            and own * tile_cols == 128
            and tile_rows % 16 == 0
            and tile_rows % own == 0
            and own & (own - 1) == 0
            and col_count % 2 == 0
            and row_count * tile_rows == col_count * tile_cols
        )
        return fused(row_count, col_count, *args) if fits else on_device(*args)

    return jax.shard_map(
        step,
        mesh=mesh,
        in_specs=(P("row", "col", None), P("row", "col"), P(), P(), P(), P(), P(), P(), P()),
        out_specs=P("row", "col", None),
        check_vma=False,
    )
```
